32 devices in a mesh: gy: 4 (over z), gx: 8 (over y, x, core).
Axes of the slice: x: 2, y: 2, z: 4, core: 2. Of those that a mesh axis runs over, the one named last changes fastest.
Arguments:
- height: float32 [384, 512], P('gx', 'gy'), may hold values from -6 to 6
- east_speed: float32 [384, 512], P('gx', 'gy'), may hold values from -3 to 3
- north_speed: float32 [384, 512], P('gx', 'gy'), may hold values from -3 to 3
- water_depth: float32 [384, 512], P('gx', 'gy'), may hold values from 0.5 to 2
- ocean_mask: int32 [384, 512], P('gx', 'gy'), may hold values 0 or 1
- fold_partner: int32 [8], replicated, may hold values from 0 to 7, each once
- love_factor: float32 [360], replicated, may hold values from 0.1 to 1
Outputs:
- sal_field: float32 [384, 512], P('gx', 'gy')
- east_next: float32 [384, 512], P('gx', 'gy')
- north_next: float32 [384, 512], P('gx', 'gy')
- height_next: float32 [384, 512], P('gx', 'gy')
The draws below stay inside these ranges and needn't reach their ends.
Inputs may be any that keep to these rules, and one draw needn't show every extreme that they name: `fold_partner`: a permutation of the tile columns.
All inputs are finite; a program needn't handle non-finite values. No bound on the sum of `ocean_mask` on one device may be relied on, other than what follows from the above.
Results may differ from the reference program's by a relative error of at most 0.00055.
Values sent between devices are 32-bit elements; how exact they have to be, the bound alone decides.
A program may use at most 64 MiB of HBM per device.

```python
import math
import jax
import jax.numpy as jnp
from jax import lax

CLON = 48
L = 360
NLON = 384
NLAT = 512
N_GX = 8


def set_ends(entries, rng, smallest, top_value):
    longest = entries.shape.index(max(entries.shape))
    spots = []
    for shift in (0, 1):
        where = [jax.random.randint(jax.random.fold_in(rng, axis), (), 0, length) for axis, length in enumerate(entries.shape)]
        where[longest] = (where[longest] + shift) % entries.shape[longest]
        spots.append(tuple(where))
    return entries.at[spots[0]].set(smallest).at[spots[1]].set(top_value)


def block_levels(key, dims, cuts, low, top_value):
    factor_of = 1.0
    for axis_at, parts in cuts:
        steps = jax.random.uniform(jax.random.fold_in(jax.random.fold_in(key, 6), axis_at), (parts,), jnp.float32, low / len(cuts), top_value / len(cuts))
        factor_of = factor_of * jnp.repeat(jnp.exp(steps), dims[axis_at] // parts).reshape((-1,) + (1,) * (len(dims) - 1 - axis_at))
    return factor_of


def noise(rng, extent, spread, reach, pieces=(), kind=jnp.bfloat16):
    array = jax.random.normal(rng, extent, jnp.float32) * spread
    if len(pieces) > 0:
        array = block_levels(rng, extent, pieces, -0.22, 0.18) * array
    return jnp.clip(array, min=-reach, max=reach).astype(kind)


def setup_inputs(seed: int = 0) -> dict:
    arg_keys = jax.random.split(jax.random.key(seed), 8)
    height = noise(arg_keys[0], (NLON, NLAT), 1.0, 6.0, ((0, 8), (1, 4)), jnp.float32)
    east_speed = noise(arg_keys[1], (NLON, NLAT), 0.5, 3.0, ((0, 8), (1, 4)), jnp.float32)
    north_speed = noise(arg_keys[2], (NLON, NLAT), 0.5, 3.0, ((0, 8), (1, 4)), jnp.float32)
    water_depth = jnp.clip(jnp.exp(math.log(2.0) - 1.3862944 * jax.random.uniform(arg_keys[3], (NLON, NLAT), jnp.float32) ** block_levels(arg_keys[3], (NLON, NLAT), ((0, 8), (1, 4)), -0.2, 0.2)), 0.5, 2.0)
    ocean_mask = set_ends((jax.random.randint(arg_keys[4], (NLON, NLAT), 0, 5) < 4).astype(jnp.int32), jax.random.fold_in(arg_keys[4], 1), 0, 1)
    fold_partner = jax.random.permutation(arg_keys[5], N_GX).astype(jnp.int32)
    love_factor = jnp.clip(jnp.exp(jax.random.uniform(arg_keys[6], (L,), jnp.float32, math.log(0.1), math.log(1.0))), 0.1, 1.0)
    return {"height": height, "east_speed": east_speed, "north_speed": north_speed, "water_depth": water_depth, "ocean_mask": ocean_mask, "fold_partner": fold_partner, "love_factor": love_factor}


COURANT = 0.35

def trig_rows(first_column, number, lon_total, degrees):
    columns = first_column + jnp.arange(number, dtype=jnp.int32)
    orders = jnp.arange(degrees, dtype=jnp.int32)
    phases = columns[:, None] * orders[None, :] % lon_total
    angles = phases.astype(jnp.float32) * (2.0 * math.pi / lon_total)
    return jnp.concatenate([jnp.cos(angles), jnp.sin(angles)], axis=1)

def latitude_rows(first_row, number, lat_total, lon_total):
    rows_float = (first_row + jnp.arange(number, dtype=jnp.int32)).astype(jnp.float32)
    colatitude = math.pi * (rows_float + 0.5) / lat_total
    sines = jnp.sin(colatitude)
    quadrature = math.pi / lat_total * (2.0 * math.pi / lon_total) * sines
    return (jnp.cos(colatitude), sines, quadrature)

def seed_values(sines, degrees):
    orders = jnp.arange(degrees, dtype=jnp.float32)
    factors = jnp.arange(1, degrees, dtype=jnp.float32)
    increments = 0.5 * jnp.log((2.0 * factors + 1.0) / (2.0 * factors))
    seed_logs = jnp.concatenate([jnp.zeros((1,), jnp.float32), jnp.cumsum(increments)])
    exponent = orders[None, :] * jnp.log(sines)[:, None] + seed_logs[None, :]
    log_shift = jnp.clip(-exponent - 80.0, 0.0, 80.0)
    return (jnp.exp(exponent + log_shift) * (1.0 / math.sqrt(4.0 * math.pi)), jnp.exp(-log_shift))

def legendre_next(carry, degree, cosines, seed_rows, orders):
    previous, before = carry
    degree_value = degree.astype(jnp.float32)
    below_value = degree_value - 1.0
    growth = jnp.sqrt(jnp.maximum(4.0 * degree_value * degree_value - 1.0, 1.0) / jnp.maximum(degree_value * degree_value - orders * orders, 1.0))
    damping = jnp.sqrt(jnp.maximum(below_value * below_value - orders * orders, 0.0) / jnp.maximum(4.0 * below_value * below_value - 1.0, 1.0))
    stepped = growth[None, :] * (cosines[:, None] * previous - damping[None, :] * before)
    values = jnp.where(degree_value == orders[None, :], seed_rows, jnp.where(degree_value > orders[None, :], stepped, 0.0))
    return ((values, previous), values)

def reference(height, east_speed, north_speed, water_depth, ocean_mask, fold_partner, love_factor):
    lon_count = height.shape[0]
    lat_count = height.shape[1]
    degrees = love_factor.shape[0]
    wet_cells = ocean_mask.astype(jnp.float32)
    surface = wet_cells * height
    cosines, sines, quadrature = latitude_rows(0, lat_count, lat_count, lon_count)
    trig = trig_rows(0, lon_count, lon_count, degrees)
    fourier = lax.dot_general(surface, trig, (((0,), (0,)), ((), ())), precision=lax.Precision.HIGHEST)
    weighted = fourier * quadrature[:, None]
    orders = jnp.arange(degrees, dtype=jnp.float32)
    seed_rows, unscale = seed_values(sines, degrees)
    empty = jnp.zeros((lat_count, degrees), jnp.float32)

    def analyse(carry, degree):
        recurrence, scaled_values = legendre_next(carry, degree, cosines, seed_rows, orders)
        values = scaled_values * unscale
        cos_part = lax.optimization_barrier(jnp.sum(values * weighted[:, :degrees], axis=0))
        sin_part = lax.optimization_barrier(jnp.sum(values * weighted[:, degrees:], axis=0))
        return (recurrence, jnp.stack([cos_part, sin_part]))
    degree_list = jnp.arange(degrees, dtype=jnp.int32)
    finished, spectrum = lax.scan(analyse, (empty, empty), degree_list)
    multiplicity = jnp.where(jnp.arange(degrees) == 0, 1.0, 2.0).astype(jnp.float32)
    scaled = spectrum * love_factor[:, None, None] * multiplicity[None, None, :]

    def synthesise(carry, inputs):
        degree, coeff_rows = inputs
        recurrence, scaled_values = legendre_next(carry[0], degree, cosines, seed_rows, orders)
        values = scaled_values * unscale
        total = carry[1] + jnp.concatenate([values * coeff_rows[0][None, :], values * coeff_rows[1][None, :]], axis=1)
        return ((recurrence, total), None)
    start_total = jnp.zeros((lat_count, 2 * degrees), jnp.float32)
    (finished_two, grid_terms), unused = lax.scan(synthesise, ((empty, empty), start_total), (degree_list, scaled))
    sal_field = lax.dot_general(trig, grid_terms, (((1,), (1,)), ((), ())), precision=lax.Precision.HIGHEST)
    pressure = surface - sal_field
    columns = jnp.arange(lon_count, dtype=jnp.int32)
    partner_columns = fold_partner[columns // CLON] * CLON + (CLON - 1 - columns % CLON)

    def north_of(field):
        return jnp.concatenate([field[:, 1:], field[partner_columns, lat_count - 1][:, None]], axis=1)

    def east_of(field):
        return jnp.roll(field, -1, axis=0)
    east_next = wet_cells * east_of(wet_cells) * (east_speed - COURANT * (east_of(pressure) - pressure))
    north_next = wet_cells * north_of(wet_cells) * (north_speed - COURANT * (north_of(pressure) - pressure))
    east_flux = 0.5 * (water_depth + east_of(water_depth)) * east_next
    north_flux = 0.5 * (water_depth + north_of(water_depth)) * north_next
    west_flux = jnp.roll(east_flux, 1, axis=0)
    south_flux = jnp.concatenate([jnp.zeros((lon_count, 1), jnp.float32), north_flux[:, :-1]], axis=1)
    height_next = wet_cells * (surface - COURANT * (east_flux - west_flux + north_flux - south_flux))
    return (sal_field, east_next, north_next, height_next)
```

```python
import functools
import math

import jax
import jax.numpy as jnp
import numpy as np
from jax import lax
from jax.experimental import pallas as pl
from jax.experimental.pallas import tpu as pltpu
from jax.sharding import PartitionSpec as P

COURANT = 0.35
CHUNK = 16
F32 = jnp.float32
BF16 = jnp.bfloat16


def split(x):
    high = x.astype(BF16)
    return high, (x - high.astype(F32)).astype(BF16)


def flip_lanes(x):
    n = x.shape[1]
    i = lax.broadcasted_iota(jnp.int32, (n, n), 0)
    j = lax.broadcasted_iota(jnp.int32, (n, n), 1)
    anti = (i + j == n - 1).astype(F32)
    return jnp.dot(x, anti, precision=lax.Precision.HIGHEST, preferred_element_type=F32)


def fill_table(dims, lat_ref, picked_ref, root_ref, ratio_ref, hi_ref, lo_ref):
    gx, gy, per, sp, degrees = dims
    half = lat_ref.shape[1]
    base = (lax.axis_index("gx") * gy + lax.axis_index("gy")) * per
    orders = (base + lax.broadcasted_iota(jnp.int32, (sp, 128), 0)).astype(F32)
    squares = orders * orders
    widen = lambda x: jnp.concatenate([x] * (half // 128), axis=1)
    cosines = jnp.broadcast_to(lat_ref[0:1, :], (sp, half))
    exponent = widen(orders) * lat_ref[1:2, :] + widen(picked_ref[...])
    log_shift = jnp.clip(-exponent - 80.0, 0.0, 80.0)
    slot = lax.broadcasted_iota(jnp.int32, (sp, half), 0)
    scale = 1.0 / math.sqrt(4.0 * math.pi)
    seeds = jnp.where(slot < per, jnp.exp(exponent + log_shift) * scale, 0.0)
    unscale = jnp.exp(-log_shift)

    def block(number, carry):
        previous, before, below = carry
        for inner in range(8):
            degree = number * 8 + inner
            value = degree.astype(F32)
            gap = value * value - squares
            inverse = lax.rsqrt(jnp.maximum(gap, 1.0))
            growth = root_ref[degree] * inverse
            damping = ratio_ref[degree] * inverse * below
            stepped = (widen(growth) * cosines) * previous - widen(damping) * before
            values = jnp.where(widen(orders) == value, seeds, stepped)
            high, low = split(values * unscale)
            rows = pl.ds(pl.multiple_of(degree * sp, sp), sp)
            hi_ref[rows, :] = high
            lo_ref[rows, :] = low
            previous, before, below = values, previous, jnp.maximum(gap, 0.0) * inverse
        return previous, before, below

    empty = jnp.zeros((sp, half), F32)
    lax.fori_loop(0, degrees // 8, block, (empty, empty, jnp.zeros((sp, 128), F32)))


def transform(dims, bands, lat_ref, love_ref, hi_ref, lo_ref):
    gx, gy, per, sp, degrees = dims
    half = lat_ref.shape[1]
    base = (lax.axis_index("gx") * gy + lax.axis_index("gy")) * per
    weights = lat_ref[2:3, :]
    mirrored = flip_lanes(jnp.concatenate(bands[gy // 2 :], axis=0))
    rows = 2 * sp
    near = jnp.concatenate(bands[: gy // 2], axis=1)
    far = jnp.concatenate(
        [mirrored[b * rows : (b + 1) * rows] for b in reversed(range(gy // 2))], axis=1
    )
    folded = jnp.concatenate([(near + far) * weights, (near - far) * weights], axis=0)
    f_hi, f_lo = split(folded)
    f_both = jnp.concatenate([f_hi, f_lo], axis=0)
    total = 2 * rows
    span = CHUNK * sp
    row = lax.broadcasted_iota(jnp.int32, (total, span), 0)
    column = lax.broadcasted_iota(jnp.int32, (total, span), 1)
    slot = row % sp
    order = base + slot
    same = (slot == column % sp) & ((column // sp + order) % 2 == row // rows)
    mask = jnp.where(same, jnp.where(order == 0, 1.0, 2.0), 0.0).astype(F32)
    nt = (((1,), (1,)), ((), ()))
    nn = (((1,), (0,)), ((), ()))
    dot = functools.partial(lax.dot_general, preferred_element_type=F32)

    def chunk(number, acc):
        at = pl.ds(pl.multiple_of(number * span, span), span)
        p_hi = hi_ref[at, :]
        p_lo = lo_ref[at, :]
        wide = dot(f_both, p_hi, nt)
        spectrum = wide[:total] + wide[total:] + dot(f_hi, p_lo, nt)
        c_hi, c_lo = split(spectrum * mask * love_ref[pl.ds(number, 1), :])
        back = dot(jnp.concatenate([c_hi, c_lo], axis=0), p_hi, nn)
        return acc + (back[:total] + back[total:] + dot(c_hi, p_lo, nn))

    acc = lax.fori_loop(0, degrees // CHUNK, chunk, jnp.zeros((total, half), F32))
    north = acc[:rows] + acc[rows:]
    south = acc[:rows] - acc[rows:]
    out = [north[:, b * 128 : (b + 1) * 128] for b in range(gy // 2)]
    for b in reversed(range(gy // 2)):
        out.append(flip_lanes(south[:, b * 128 : (b + 1) * 128]))
    return out


def legendre_kernel(dims, f_ref, lat_ref, picked_ref, love_ref, root_ref, ratio_ref, g_ref, hi_ref, lo_ref):
    fill_table(dims, lat_ref, picked_ref, root_ref, ratio_ref, hi_ref, lo_ref)
    bands = [f_ref[b] for b in range(dims[1])]
    for b, out in enumerate(transform(dims, bands, lat_ref, love_ref, hi_ref, lo_ref)):
        g_ref[b] = out


def trig(orders, columns, is_sine, lon_count):
    phase = (orders * columns + is_sine * (lon_count // 4 * 3)) % lon_count
    return jnp.cos(phase.astype(F32) * (2.0 * math.pi / lon_count))


def on_device(height, east_speed, north_speed, water_depth, ocean_mask, fold_partner, love_factor):
    tile_lon, tile_lat = height.shape
    degrees = love_factor.shape[0]
    gx = lax.axis_size("gx")
    gy = lax.axis_size("gy")
    x = lax.axis_index("gx")
    y = lax.axis_index("gy")
    lon_count = tile_lon * gx
    lat_count = tile_lat * gy
    half = lat_count // 2
    per = -(-degrees // (gx * gy))
    sp = -(-per // 16) * 16
    padded = -(-degrees // CHUNK) * CHUNK
    dims = (gx, gy, per, sp, padded)
    rows = 2 * sp
    wet = ocean_mask.astype(F32)
    surface = wet * height
    is_top = y == gy - 1

    def lanes(v):
        return jnp.pad(v, ((0, 0), (0, tile_lat - v.shape[1])))

    top = lanes(jnp.stack([wet[:, -1], surface[:, -1], water_depth[:, -1], north_speed[:, -1]]))
    low = lanes(jnp.stack([wet[:, 0], surface[:, 0], water_depth[:, 0]]))
    pack = jnp.concatenate(
        [
            surface,
            wet[:1], water_depth[:1],
            wet[-1:], water_depth[-1:], east_speed[-1:],
            top[:3],
        ],
        axis=0,
    )
    gathered = lax.all_gather(pack, "gx", axis=0)

    slot_rows = jnp.arange(gy * rows, dtype=jnp.int32)
    slot = slot_rows % sp
    sine = slot_rows // sp % 2
    group_orders = (x * gy + slot_rows // rows) * per + slot
    columns = jnp.arange(lon_count, dtype=jnp.int32)
    valid = (slot < per).astype(F32)
    ahead = trig(group_orders[:, None], columns[None, :], sine[:, None], lon_count) * valid[:, None]
    ext = tile_lon + 8
    place = jnp.arange(gx * ext, dtype=jnp.int32)
    within = place % ext
    offset = jnp.where(within <= tile_lon, within, jnp.where(within == tile_lon + 1, -1, 0))
    ext_columns = (place // ext * tile_lon + offset + lon_count) % lon_count
    behind = trig(group_orders[None, :], ext_columns[:, None], sine[None, :], lon_count) * valid[None, :]

    band_rows = jnp.dot(
        ahead, gathered[:, :tile_lon].reshape(lon_count, tile_lat),
        precision=lax.Precision.HIGH, preferred_element_type=F32,
    ).reshape(gy, rows, tile_lat)
    edges = jnp.concatenate([top, low, jnp.zeros((1, tile_lat), F32)], axis=0)
    sent = jnp.concatenate([band_rows, jnp.broadcast_to(edges, (gy,) + edges.shape)], axis=1)
    came = lax.all_to_all(sent, "gy", split_axis=0, concat_axis=0, tiled=True)

    theta = np.pi * (np.arange(half) + 0.5) / lat_count
    quadrature = np.pi / lat_count * (2.0 * np.pi / lon_count) * np.sin(theta)
    lat_table = np.zeros((8, half), np.float32)
    lat_table[0], lat_table[1], lat_table[2] = np.cos(theta), np.log(np.sin(theta)), quadrature
    slots = per * gx * gy + sp
    k = np.arange(1, slots, dtype=np.float64)
    logs = np.concatenate([[0.0], np.cumsum(0.5 * np.log((2.0 * k + 1.0) / (2.0 * k)))])
    first = (x * gy + y) * per
    picked = lax.dynamic_slice(jnp.asarray(logs.astype(np.float32)), (first,), (sp,))
    picked = jnp.broadcast_to(picked[:, None], (sp, 128))
    ell = np.arange(padded, dtype=np.float64)
    root = np.sqrt(np.maximum(4.0 * ell * ell - 1.0, 1.0))
    ratio = root / np.sqrt(np.maximum(4.0 * (ell - 1.0) ** 2 - 1.0, 1.0))
    love = jnp.repeat(jnp.pad(love_factor, (0, padded - degrees)), sp).reshape(padded // CHUNK, CHUNK * sp)

    vmem = pl.BlockSpec(memory_space=pltpu.VMEM)
    smem = pl.BlockSpec(memory_space=pltpu.SMEM)
    grid_rows = pl.pallas_call(
        functools.partial(legendre_kernel, dims),
        out_shape=jax.ShapeDtypeStruct((gy, rows, tile_lat), F32),
        in_specs=[vmem, vmem, vmem, vmem, smem, smem],
        out_specs=vmem,
        scratch_shapes=[
            pltpu.VMEM((padded * sp, half), BF16),
            pltpu.VMEM((padded * sp, half), BF16),
        ],
        compiler_params=pltpu.CompilerParams(vmem_limit_bytes=40 * 2**20),
    )(
        came[:, :rows], jnp.asarray(lat_table), picked, love,
        jnp.asarray(root.astype(np.float32)), jnp.asarray(ratio.astype(np.float32)),
    )
    norths = jnp.concatenate([grid_rows[1:, :, :1], jnp.zeros((1, rows, 1), F32)], axis=0)
    souths = jnp.concatenate([jnp.zeros((1, rows, 1), F32), grid_rows[:-1, :, -1:]], axis=0)
    rims = jnp.concatenate([norths, souths], axis=2)
    rims = jnp.pad(jnp.swapaxes(rims, 1, 2), ((0, 0), (0, 6), (0, tile_lat - rows)))
    back = lax.all_to_all(
        jnp.concatenate([grid_rows, rims], axis=1), "gy", split_axis=0, concat_axis=0, tiled=True
    )
    terms = back[:, :rows].reshape(gy * rows, tile_lat)
    rim_terms = jnp.swapaxes(back[:, rows : rows + 2, :rows], 1, 2).reshape(gy * rows, 2)
    made = jnp.dot(
        behind, jnp.concatenate([terms, rim_terms], axis=1),
        precision=lax.Precision.HIGH, preferred_element_type=F32,
    ).reshape(gx, ext, tile_lat + 2)
    folded = made[:, :tile_lon, tile_lat - 1][fold_partner][:, ::-1]
    north_rim = jnp.where(is_top, folded, made[:, :tile_lon, tile_lat])
    south_rim = made[:, :tile_lon, tile_lat + 1]
    rim = jnp.stack([north_rim, south_rim], axis=1)
    rim = jnp.pad(rim, ((0, 0), (0, 6), (0, tile_lat - tile_lon)))
    parts = lax.all_to_all(
        jnp.concatenate([made[:, :, :tile_lat], rim], axis=1), "gx", split_axis=0, concat_axis=0, tiled=True
    )
    sal_all = jnp.sum(parts.reshape(gx, ext + 8, tile_lat), axis=0)
    sal = sal_all[:tile_lon]

    east_of = lax.dynamic_index_in_dim(gathered, (x + 1) % gx, 0, False)
    west_of = lax.dynamic_index_in_dim(gathered, (x + gx - 1) % gx, 0, False)
    fold_of = lax.dynamic_index_in_dim(gathered, fold_partner[x], 0, False)[tile_lon + 5 :, :tile_lon][:, ::-1]
    north_of = came[jnp.minimum(y + 1, gy - 1), rows + 4 : rows + 7, :tile_lon]
    north_of = jnp.where(is_top, fold_of, north_of)
    south_of = came[jnp.maximum(y - 1, 0), rows : rows + 4, :tile_lon]

    pressure = surface - sal
    east_p = east_of[:1] - sal_all[tile_lon : tile_lon + 1]
    west_p = west_of[tile_lon - 1 : tile_lon] - sal_all[tile_lon + 1 : tile_lon + 2]
    north_p = north_of[1] - sal_all[ext, :tile_lon]
    south_p = south_of[1] - sal_all[ext + 1, :tile_lon]

    cat = functools.partial(jnp.concatenate, axis=0)
    p_x = cat([west_p, pressure, east_p])
    w_x = cat([west_of[tile_lon + 2 : tile_lon + 3], wet, east_of[tile_lon : tile_lon + 1]])
    d_x = cat([west_of[tile_lon + 3 : tile_lon + 4], water_depth, east_of[tile_lon + 1 : tile_lon + 2]])
    u_x = cat([west_of[tile_lon + 4 : tile_lon + 5], east_speed])
    east = w_x[:-1] * w_x[1:] * (u_x - COURANT * (p_x[1:] - p_x[:-1]))
    east_flux = 0.5 * (d_x[:-1] + d_x[1:]) * east
    cat = lambda parts: jnp.concatenate(parts, axis=1)
    p_y = cat([south_p[:, None], pressure, north_p[:, None]])
    w_y = cat([south_of[0][:, None], wet, north_of[0][:, None]])
    d_y = cat([south_of[2][:, None], water_depth, north_of[2][:, None]])
    v_y = cat([south_of[3][:, None], north_speed])
    north = w_y[:, :-1] * w_y[:, 1:] * (v_y - COURANT * (p_y[:, 1:] - p_y[:, :-1]))
    north_flux = 0.5 * (d_y[:, :-1] + d_y[:, 1:]) * north
    gate = jnp.where(y > 0, 1.0, 0.0).astype(F32)
    south_flux = cat([north_flux[:, :1] * gate, north_flux[:, 1:-1]])
    height_next = wet * (
        surface - COURANT * (east_flux[1:] - east_flux[:-1] + north_flux[:, 1:] - south_flux)
    )
    return sal, east[1:], north[:, 1:], height_next


def solution(mesh):
    spec = P("gx", "gy")
    return jax.shard_map(
        on_device, mesh=mesh, in_specs=(spec,) * 5 + (P(), P()), out_specs=(spec,) * 4, check_vma=False
    )
```

```python
import functools
import math

import jax
import jax.numpy as jnp
import numpy as np
from jax import lax
from jax.experimental import pallas as pl
from jax.experimental.pallas import tpu as pltpu
from jax.sharding import PartitionSpec as P

COURANT = 0.35
CHUNK = 16
F32 = jnp.float32
BF16 = jnp.bfloat16


def split(x):
    high = x.astype(BF16)
    return high, (x - high.astype(F32)).astype(BF16)


def flip_lanes(x):
    n = x.shape[1]
    i = lax.broadcasted_iota(jnp.int32, (n, n), 0)
    j = lax.broadcasted_iota(jnp.int32, (n, n), 1)
    anti = (i + j == n - 1).astype(F32)
    return jnp.dot(x, anti, precision=lax.Precision.HIGHEST, preferred_element_type=F32)


def fill_table(dims, lat_ref, logs_ref, root_ref, ratio_ref, hi_ref, lo_ref):
    gx, gy, per, sp, degrees = dims
    half = lat_ref.shape[1]
    base = (lax.axis_index("gx") * gy + lax.axis_index("gy")) * per
    orders = (base + lax.broadcasted_iota(jnp.int32, (sp, 128), 0)).astype(F32)
    squares = orders * orders
    widen = lambda x: jnp.concatenate([x] * (half // 128), axis=1)
    cosines = jnp.broadcast_to(lat_ref[0:1, :], (sp, half))
    slot_row = lax.broadcasted_iota(jnp.int32, (sp, 128), 0)
    picked = jnp.zeros((sp, 128), F32)
    for s in range(per):
        picked = jnp.where(slot_row == s, logs_ref[base + s], picked)
    exponent = widen(orders) * lat_ref[1:2, :] + widen(picked)
    log_shift = jnp.clip(-exponent - 80.0, 0.0, 80.0)
    slot = lax.broadcasted_iota(jnp.int32, (sp, half), 0)
    scale = 1.0 / math.sqrt(4.0 * math.pi)
    seeds = jnp.where(slot < per, jnp.exp(exponent + log_shift) * scale, 0.0)
    unscale = jnp.exp(-log_shift)

    def block(number, carry):
        previous, before, below = carry
        for inner in range(8):
            degree = number * 8 + inner
            value = degree.astype(F32)
            gap = value * value - squares
            inverse = lax.rsqrt(jnp.maximum(gap, 1.0))
            growth = root_ref[degree] * inverse
            damping = ratio_ref[degree] * inverse * below
            stepped = (widen(growth) * cosines) * previous - widen(damping) * before
            values = jnp.where(widen(orders) == value, seeds, stepped)
            high, low = split(values * unscale)
            rows = pl.ds(pl.multiple_of(degree * sp, sp), sp)
            hi_ref[rows, :] = high
            lo_ref[rows, :] = low
            previous, before, below = values, previous, jnp.maximum(gap, 0.0) * inverse
        return previous, before, below

    empty = jnp.zeros((sp, half), F32)
    start = (empty, empty, jnp.zeros((sp, 128), F32))
    return lambda first, last, carry=start: lax.fori_loop(first, last, block, carry)


def transform(dims, bands, lat_ref, love_ref, hi_ref, lo_ref):
    known = love_ref.shape[0]
    gx, gy, per, sp, degrees = dims
    half = lat_ref.shape[1]
    base = (lax.axis_index("gx") * gy + lax.axis_index("gy")) * per
    weights = lat_ref[2:3, :]
    mirrored = flip_lanes(jnp.concatenate(bands[gy // 2 :], axis=0))
    rows = 2 * sp
    near = jnp.concatenate(bands[: gy // 2], axis=1)
    far = jnp.concatenate(
        [mirrored[b * rows : (b + 1) * rows] for b in reversed(range(gy // 2))], axis=1
    )
    folded = jnp.concatenate([(near + far) * weights, (near - far) * weights], axis=0)
    f_hi, f_lo = split(folded)
    f_both = jnp.concatenate([f_hi, f_lo], axis=0)
    total = 2 * rows
    span = CHUNK * sp
    row = lax.broadcasted_iota(jnp.int32, (total, span), 0)
    column = lax.broadcasted_iota(jnp.int32, (total, span), 1)
    slot = row % sp
    order = base + slot
    same = (slot == column % sp) & ((column // sp + order) % 2 == row // rows)
    mask = jnp.where(same, jnp.where(order == 0, 1.0, 2.0), 0.0).astype(F32)
    nt = (((1,), (1,)), ((), ()))
    nn = (((1,), (0,)), ((), ()))
    dot = functools.partial(lax.dot_general, preferred_element_type=F32)

    lane = lax.broadcasted_iota(jnp.int32, (1, span), 1)

    def chunk(number, acc):
        love = jnp.zeros((1, span), F32)
        for k in range(CHUNK):
            degree = number * CHUNK + k
            factor = love_ref[jnp.minimum(degree, known - 1)] * (degree < known).astype(F32)
            love = jnp.where(lane // sp == k, factor, love)
        at = pl.ds(pl.multiple_of(number * span, span), span)
        p_hi = hi_ref[at, :]
        p_lo = lo_ref[at, :]
        wide = dot(f_both, p_hi, nt)
        spectrum = wide[:total] + wide[total:] + dot(f_hi, p_lo, nt)
        c_hi, c_lo = split(spectrum * mask * love)
        back = dot(jnp.concatenate([c_hi, c_lo], axis=0), p_hi, nn)
        return acc + (back[:total] + back[total:] + dot(c_hi, p_lo, nn))

    acc = lax.fori_loop(0, degrees // CHUNK, chunk, jnp.zeros((total, half), F32))
    north = acc[:rows] + acc[rows:]
    south = acc[:rows] - acc[rows:]
    out = [north[:, b * 128 : (b + 1) * 128] for b in range(gy // 2)]
    for b in reversed(range(gy // 2)):
        out.append(flip_lanes(south[:, b * 128 : (b + 1) * 128]))
    return out


def wave(product, lon_count):
    lon = float(lon_count)
    phase = product - lon * jnp.floor((product + 0.5) * (1.0 / lon))
    y = jnp.abs(phase - lon / 2)
    z = jnp.minimum(y, lon / 2 - y) * (2.0 * math.pi / lon)
    q = z * z
    series = jnp.full_like(q, 1.0 / math.factorial(12))
    for k in (10, 8, 6, 4, 2, 0):
        series = series * q + (-1.0) ** (k // 2) / math.factorial(k)
    return jnp.where(y < lon / 4, -series, series)


def group_slots(dims, shape, axis):
    gx, gy, per, sp, degrees = dims
    index = lax.broadcasted_iota(jnp.int32, shape, axis)
    slot = index % sp
    orders = (lax.axis_index("gx") * gy + index // (2 * sp)) * per + slot
    return orders.astype(F32), (index // sp % 2).astype(F32), (slot < per).astype(F32)


def trig_ahead(dims, lon_count):
    rows = dims[1] * 2 * dims[3]
    orders, sine, valid = group_slots(dims, (rows, 128), 0)
    lane = lax.broadcasted_iota(jnp.int32, (rows, 128), 1)
    blocks = []
    for n in range(lon_count // 128):
        product = orders * (lane + 128 * n).astype(F32) + sine * (0.75 * lon_count)
        blocks.append(wave(product, lon_count) * valid)
    return jnp.concatenate(blocks, axis=1)


def trig_behind(dims, tile_lon, lon_count):
    rows = dims[1] * 2 * dims[3]
    ext = tile_lon + 8
    orders, sine, valid = group_slots(dims, (ext, rows), 1)
    within = lax.broadcasted_iota(jnp.int32, (ext, rows), 0)
    blocks = []
    for t in range(dims[0]):
        column = t * tile_lon + within
        after = (t + 1) * tile_lon % lon_count
        prior = (t * tile_lon - 1) % lon_count
        column = jnp.where(within < tile_lon, column, jnp.where(within == tile_lon, after, prior))
        blocks.append(wave(orders * column.astype(F32) + sine * (0.75 * lon_count), lon_count) * valid)
    return jnp.concatenate(blocks, axis=0)


def three_pass(left, right):
    l_hi, l_lo = split(left)
    r_hi, r_lo = split(right)
    dot = functools.partial(jnp.dot, preferred_element_type=F32)
    return dot(l_hi, r_hi) + dot(l_lo, r_hi) + dot(l_hi, r_lo)


def as_row(column, reverse=False):
    n = column.shape[0]
    i = lax.broadcasted_iota(jnp.int32, (n, 128), 0)
    j = lax.broadcasted_iota(jnp.int32, (n, 128), 1)
    chosen = (j == n - 1 - i) if reverse else (i == j)
    return jnp.sum(jnp.where(chosen, column, 0.0), axis=0, keepdims=True)


def as_column(row, n, reverse=False):
    i = lax.broadcasted_iota(jnp.int32, (n, 128), 0)
    j = lax.broadcasted_iota(jnp.int32, (n, 128), 1)
    chosen = (j == n - 1 - i) if reverse else (i == j)
    return jnp.sum(jnp.where(chosen, row, 0.0), axis=1, keepdims=True)


def step_kernel(
    dims, height_hbm, east_hbm, north_hbm, depth_hbm, mask_hbm, lat_ref,
    fold_ref, love_ref, logs_ref, root_ref, ratio_ref,
    sal_ref, east_out, north_out, next_out,
    height_ref, east_ref, north_ref, depth_ref, mask_ref,
    hi_ref, lo_ref, send1, recv1, send2, recv2, send3, recv3, send4, recv4, made_ref,
    load_sem, s1, r1, s2, r2, s3, r3, s4, r4,
):
    gx, gy, per, sp, degrees = dims
    tile_lon, tile_lat = height_ref.shape
    lon_count = gx * tile_lon
    rows = 2 * sp
    ext = tile_lon + 8
    x = lax.axis_index("gx")
    y = lax.axis_index("gy")
    loads = [
        pltpu.make_async_copy(src, dst, load_sem.at[i])
        for i, (src, dst) in enumerate(
            [
                (height_hbm, height_ref), (mask_hbm, mask_ref), (depth_hbm, depth_ref),
                (east_hbm, east_ref), (north_hbm, north_ref),
            ]
        )
    ]
    for load in loads:
        load.start()
    barrier = pltpu.get_barrier_semaphore()
    for d in range(1, gx):
        pl.semaphore_signal(barrier, 1, device_id={"gx": (x + d) % gx}, device_id_type=pl.DeviceIdType.MESH)
    for d in range(1, gy):
        pl.semaphore_signal(barrier, 1, device_id={"gy": (y + d) % gy}, device_id_type=pl.DeviceIdType.MESH)
    for load in loads:
        load.wait()

    def copies(axis, here, size, source, landing, s_sem, r_sem):
        made = []
        for d in range(1, size):
            peer = (here + d) % size
            made.append(
                pltpu.make_async_remote_copy(
                    src_ref=source(peer), dst_ref=landing.at[here], send_sem=s_sem.at[peer],
                    recv_sem=r_sem.at[here], device_id={axis: peer},
                    device_id_type=pl.DeviceIdType.MESH,
                )
            )
        return made

    def arrive(axis, here, size, source, landing, s_sem, r_sem):
        for d in range(1, size):
            peer = (here + d) % size
            pltpu.make_async_remote_copy(
                src_ref=source(peer), dst_ref=landing.at[peer], send_sem=s_sem.at[peer],
                recv_sem=r_sem.at[peer], device_id={axis: peer},
                device_id_type=pl.DeviceIdType.MESH,
            ).wait_recv()

    wet = mask_ref[...].astype(F32)
    surface = wet * height_ref[...]
    depth = depth_ref[...]
    east_speed = east_ref[...]
    north_speed = north_ref[...]
    last = slice(tile_lat - 1, tile_lat)
    top = [as_row(v[:, last]) for v in (wet, surface, depth, north_speed)]
    low = [as_row(v[:, :1]) for v in (wet, surface, depth)]
    end = slice(tile_lon - 1, tile_lon)
    pack = jnp.concatenate(
        [surface, wet[:1], depth[:1], wet[end], depth[end], east_speed[end]] + top[:3], axis=0
    )
    send1[...] = pack
    recv1[x] = pack
    pl.semaphore_wait(barrier, gx + gy - 2)
    way1 = ("gx", x, gx, lambda peer: send1, recv1, s1, r1)
    out1 = copies(*way1)
    for c in out1:
        c.start()
    ahead = trig_ahead(dims, lon_count)
    fill = fill_table(dims, lat_ref, logs_ref, root_ref, ratio_ref, hi_ref, lo_ref)
    blocks = degrees // 8
    carry = fill(0, blocks // 3)
    arrive(*way1)
    every = jnp.concatenate([recv1[t, :tile_lon, :] for t in range(gx)], axis=0)
    band = three_pass(ahead, every)
    edges = jnp.concatenate(top + low + [jnp.zeros((1, tile_lat), F32)], axis=0)
    for k in range(gy):
        send2[k] = jnp.concatenate([band[k * rows : (k + 1) * rows], edges], axis=0)
    way2 = ("gy", y, gy, lambda peer: send2.at[peer], recv2, s2, r2)
    out2 = copies(*way2)
    for c in out2:
        c.start()
    recv2[y] = send2[y]
    fill(blocks // 3, blocks, carry)
    arrive(*way2)
    bands = [recv2[k, :rows, :] for k in range(gy)]
    grids = transform(dims, bands, lat_ref, love_ref, hi_ref, lo_ref)
    none = jnp.zeros((1, tile_lat), F32)
    for k in range(gy):
        north_rim = as_row(grids[k + 1][:, :1]) if k + 1 < gy else none
        south_rim = as_row(grids[k - 1][:, last]) if k > 0 else none
        rims = jnp.concatenate([north_rim, south_rim, jnp.zeros((6, tile_lat), F32)], axis=0)
        send3[k] = jnp.concatenate([grids[k], rims], axis=0)
    way3 = ("gy", y, gy, lambda peer: send3.at[peer], recv3, s3, r3)
    out3 = copies(*way3)
    for c in out3:
        c.start()
    recv3[y] = send3[y]
    behind = trig_behind(dims, tile_lon, lon_count)
    arrive(*way3)
    lane = lax.broadcasted_iota(jnp.int32, (rows, 128), 1)
    terms = []
    for k in range(gy):
        north_rim = as_column(recv3[k, rows : rows + 1, :], rows)
        south_rim = as_column(recv3[k, rows + 1 : rows + 2, :], rows)
        rim = jnp.where(lane == 0, north_rim, jnp.where(lane == 1, south_rim, 0.0))
        terms.append(jnp.concatenate([recv3[k, :rows, :], rim], axis=1))
    made = three_pass(behind, jnp.concatenate(terms, axis=0))
    for t in range(gx):
        made_ref[t] = made[t * ext : (t + 1) * ext]
    is_top = y == gy - 1
    for t in range(gx):
        piece = made[t * ext : (t + 1) * ext]
        over = made_ref[fold_ref[t]]
        folded = as_row(over[:tile_lon, last], True)
        straight = as_row(piece[:tile_lon, tile_lat : tile_lat + 1])
        south_rim = as_row(piece[:tile_lon, tile_lat + 1 : tile_lat + 2])
        north_rim = jnp.where(is_top, folded, straight)
        rims = jnp.concatenate([north_rim, south_rim, jnp.zeros((6, tile_lat), F32)], axis=0)
        send4[t] = jnp.concatenate([piece[:, :tile_lat], rims], axis=0)
    way4 = ("gx", x, gx, lambda peer: send4.at[peer], recv4, s4, r4)
    out4 = copies(*way4)
    for c in out4:
        c.start()
    recv4[x] = send4[x]

    east_of = recv1[(x + 1) % gx]
    west_of = recv1[(x + gx - 1) % gx]
    fold_of = recv1[fold_ref[x]]
    north_of = recv2[jnp.minimum(y + 1, gy - 1), rows : rows + 8, :]
    south_of = recv2[jnp.maximum(y - 1, 0), rows : rows + 8, :]

    def north_column(i):
        across = as_column(fold_of[tile_lon + 5 + i : tile_lon + 6 + i], tile_lon, True)
        return jnp.where(is_top, across, as_column(north_of[4 + i : 5 + i], tile_lon))

    n_wet, n_surface, n_depth = [north_column(i) for i in range(3)]
    s_wet, s_surface, s_depth, s_speed = [as_column(south_of[i : i + 1], tile_lon) for i in range(4)]
    rows_cat = lambda parts: jnp.concatenate(parts, axis=0)
    lanes_cat = lambda parts: jnp.concatenate(parts, axis=1)
    at = lambda block, i: block[i : i + 1]
    w_east = rows_cat([wet[1:], at(east_of, tile_lon)])
    d_east = rows_cat([depth[1:], at(east_of, tile_lon + 1)])
    w_west = at(west_of, tile_lon + 2)
    d_west = at(west_of, tile_lon + 3)
    u_west = at(west_of, tile_lon + 4)
    w_north = lanes_cat([wet[:, 1:], n_wet])
    d_north = lanes_cat([depth[:, 1:], n_depth])
    arrive(*way4)
    total = recv4[0]
    for t in range(1, gx):
        total = total + recv4[t]
    sal = total[:tile_lon]
    sal_ref[...] = sal
    pressure = surface - sal
    p_east = at(east_of, 0) - at(total, tile_lon)
    p_west = at(west_of, tile_lon - 1) - at(total, tile_lon + 1)
    p_north = n_surface - as_column(at(total, ext), tile_lon)
    p_south = s_surface - as_column(at(total, ext + 1), tile_lon)
    east = wet * w_east * (east_speed - COURANT * (rows_cat([pressure[1:], p_east]) - pressure))
    east_west = w_west * wet[:1] * (u_west - COURANT * (pressure[:1] - p_west))
    east_flux = 0.5 * (depth + d_east) * east
    flux_west = 0.5 * (d_west + depth[:1]) * east_west
    north = wet * w_north * (north_speed - COURANT * (lanes_cat([pressure[:, 1:], p_north]) - pressure))
    north_south = s_wet * wet[:, :1] * (s_speed - COURANT * (pressure[:, :1] - p_south))
    north_flux = 0.5 * (depth + d_north) * north
    flux_south = jnp.where(y > 0, 0.5 * (s_depth + depth[:, :1]) * north_south, 0.0)
    east_out[...] = east
    north_out[...] = north
    next_out[...] = wet * (
        surface
        - COURANT
        * (
            east_flux
            - rows_cat([flux_west, east_flux[:-1]])
            + north_flux
            - lanes_cat([flux_south, north_flux[:, :-1]])
        )
    )
    for c in out1 + out2 + out3 + out4:
        c.wait_send()


def on_device(height, east_speed, north_speed, water_depth, ocean_mask, fold_partner, love_factor):
    tile_lon, tile_lat = height.shape
    degrees = love_factor.shape[0]
    gx = lax.axis_size("gx")
    gy = lax.axis_size("gy")
    lon_count = tile_lon * gx
    lat_count = tile_lat * gy
    half = lat_count // 2
    per = -(-degrees // (gx * gy))
    sp = -(-per // 16) * 16
    padded = -(-degrees // CHUNK) * CHUNK
    dims = (gx, gy, per, sp, padded)
    rows = 2 * sp
    ext = tile_lon + 8

    theta = np.pi * (np.arange(half) + 0.5) / lat_count
    quadrature = np.pi / lat_count * (2.0 * np.pi / lon_count) * np.sin(theta)
    lat_table = np.zeros((8, half), np.float32)
    lat_table[0], lat_table[1], lat_table[2] = np.cos(theta), np.log(np.sin(theta)), quadrature
    slots = per * gx * gy
    k = np.arange(1, slots, dtype=np.float64)
    logs = np.concatenate([[0.0], np.cumsum(0.5 * np.log((2.0 * k + 1.0) / (2.0 * k)))])
    ell = np.arange(padded, dtype=np.float64)
    root = np.sqrt(np.maximum(4.0 * ell * ell - 1.0, 1.0))
    ratio = root / np.sqrt(np.maximum(4.0 * (ell - 1.0) ** 2 - 1.0, 1.0))

    hbm = pl.BlockSpec(memory_space=pl.ANY)
    vmem = pl.BlockSpec(memory_space=pltpu.VMEM)
    smem = pl.BlockSpec(memory_space=pltpu.SMEM)
    tile = lambda *lead: pltpu.VMEM(lead + (tile_lat,), F32)
    dma = lambda n: pltpu.SemaphoreType.DMA((n,))
    return pl.pallas_call(
        functools.partial(step_kernel, dims),
        out_shape=[jax.ShapeDtypeStruct(height.shape, F32)] * 4,
        in_specs=[hbm] * 5 + [vmem] + [smem] * 5,
        out_specs=[vmem] * 4,
        scratch_shapes=[
            tile(tile_lon), tile(tile_lon), tile(tile_lon), tile(tile_lon),
            pltpu.VMEM((tile_lon, tile_lat), jnp.int32),
            pltpu.VMEM((padded * sp, half), BF16),
            pltpu.VMEM((padded * sp, half), BF16),
            tile(ext), tile(gx, ext),
            tile(gy, rows + 8), tile(gy, rows + 8),
            tile(gy, rows + 8), tile(gy, rows + 8),
            tile(gx, ext + 8), tile(gx, ext + 8),
            pltpu.VMEM((gx, ext, 2 * tile_lat), F32),
            dma(5), dma(gx), dma(gx), dma(gy), dma(gy), dma(gy), dma(gy), dma(gx), dma(gx),
        ],
        compiler_params=pltpu.CompilerParams(
            collective_id=0, has_side_effects=True, vmem_limit_bytes=48 * 2**20
        ),
    )(
        height, east_speed, north_speed, water_depth, ocean_mask, jnp.asarray(lat_table),
        fold_partner, love_factor,
        *(jnp.asarray(a.astype(np.float32)) for a in (logs, root, ratio)),
    )


def solution(mesh):
    spec = P("gx", "gy")
    return jax.shard_map(
        on_device, mesh=mesh, in_specs=(spec,) * 5 + (P(), P()), out_specs=(spec,) * 4, check_vma=False
    )
```
